64 devices in a mesh: rep: 4 (over x, y), dp: 16 (over z, core).
Axes of the slice: x: 2, y: 2, z: 8, core: 2. Of those that a mesh axis runs over, the one named last changes fastest.
The devices are a block of a 4x4x8 slice.
Arguments:
- a: bfloat16 [64, 4, 8192, 512], P(('rep', 'dp')), parts along dimension 0
- g: bfloat16 [64, 4, 8192, 1280], P(('rep', 'dp')), parts along dimension 0
Outputs:
- output: bfloat16 [16, 512, 1280], P('rep'), parts along dimension 0
There are 4 independent parts. The reference program is written for one: setup_inputs(seed, part) draws one part's arguments, and reference() takes and returns one part's arrays. A program takes and returns all parts, laid end to end along the dimension named above; each array names one.
All inputs are finite; a program needn't handle non-finite values.
Results may differ from the reference program's by a relative error of at most 0.012.
Values are sent between devices in bfloat16 or wider.
A program may use at most 768 MiB of HBM per device.

```python
import jax
import jax.numpy as jnp
from jax import lax

DEVICES = 16
MATRICES = 4
TOKENS = 8192
D = 512
FF = 1280


def setup_inputs(seed: int = 0, part: int = 0) -> dict:
    ka, kg, ks = (jax.random.fold_in(k, part) for k in jax.random.split(jax.random.key(seed), 3))
    size = 2.0 ** jax.random.uniform(ks, (DEVICES, MATRICES, 1, 1), jnp.float32, -1.0, 1.0)
    a = jax.random.normal(ka, (DEVICES, MATRICES, TOKENS, D), jnp.float32)
    g = size * jax.random.normal(kg, (DEVICES, MATRICES, TOKENS, FF), jnp.float32) * (DEVICES * TOKENS) ** -0.5
    return {"a": a.astype(jnp.bfloat16), "g": g.astype(jnp.bfloat16)}


def reference(a, g):
    def take(so_far, one):
        return so_far + jnp.einsum("ntd,ntf->ndf", *one, preferred_element_type=jnp.float32), None

    return lax.scan(take, jnp.zeros((MATRICES, D, FF), jnp.float32), (a, g))[0].astype(jnp.bfloat16)
```

```python
import functools

import jax
import jax.numpy as jnp
from jax import lax
from jax.experimental import pallas as pl
from jax.experimental.pallas import tpu as pltpu

BF16, F32 = jnp.bfloat16, jnp.float32
COLS = 256
TOKS = 2048
DEPTH = 3
LAG = 2


def sums_kernel(chips, a_ref, g_ref, o_ref, a_in, a_t, g_in, acc, own, x_tx, x_rx, r_tx, r_rx, res,
                a_sem, g_sem, o_sem, x_send, x_recv, r_send, r_recv, q_send, q_recv, f_send, f_recv):
    mats, toks, d = a_ref.shape
    per = g_ref.shape[2] // COLS
    steps = toks // TOKS
    pieces = mats * per
    half = d // 2
    rows = half // chips
    hops = chips // 2

    rep, me = lax.axis_index("rep"), lax.axis_index("dp")
    chip, core = me // 2, lax.rem(me, 2)

    def at(z, c):
        return (rep, lax.rem(z + chips, chips) * 2 + c)

    partner, up, down = at(chip, 1 - core), at(chip + 1, core), at(chip - 1, core)
    ahead = (up, down)
    sign = (1, -1)

    barrier = pltpu.get_barrier_semaphore()
    for dev in (partner, up, down):
        pl.semaphore_signal(barrier, inc=1, device_id=dev, device_id_type=pl.DeviceIdType.MESH)
    pl.semaphore_wait(barrier, 3)

    def remote(src, dst, ss, rs, dev):
        return pltpu.make_async_remote_copy(src_ref=src, dst_ref=dst, send_sem=ss, recv_sem=rs, device_id=dev,
                                            device_id_type=pl.DeviceIdType.MESH)

    def each(lo, hi, f):
        def body(i, carry):
            f(i)
            return carry
        lax.fori_loop(lo, hi, body, 0)

    def a_copy(n, k):
        ks = pl.ds(pl.multiple_of(k * TOKS, TOKS), TOKS)
        return pltpu.make_async_copy(a_ref.at[n, ks, :], a_in.at[ks, :], a_sem.at[k])

    def g_copy(c, k):
        ks = pl.ds(pl.multiple_of(k * TOKS, TOKS), TOKS)
        cs = pl.ds(pl.multiple_of((c % per) * COLS, COLS), COLS)
        s = lax.rem(c, DEPTH)
        return pltpu.make_async_copy(g_ref.at[c // per, ks, cs], g_in.at[s, ks, :], g_sem.at[s, k])

    def o_copy(c):
        cs = pl.ds(pl.multiple_of((c % per) * COLS, COLS), COLS)
        return pltpu.make_async_copy(res.at[c], o_ref.at[c // per, :, cs], o_sem.at[c])

    def half_rows(which):
        return pl.ds(pl.multiple_of(which * half, half), half)

    def shard(z, part=None):
        z = lax.rem(z + chips, chips)
        n = rows if part is None else rows // 2
        return pl.ds(pl.multiple_of(z * rows + (0 if part is None else part * n), n), n)

    def res_rows(z, c, part=None):
        z = lax.rem(z + chips, chips)
        n = rows if part is None else rows // 2
        return pl.ds(pl.multiple_of(c * half + z * rows + (0 if part is None else part * n), n), n)

    h = rows // 2

    def x_copy(c):
        return remote(x_tx.at[c], x_rx.at[c], x_send.at[c], x_recv.at[c], partner)

    def r_copy(c, way, s):
        n = h if s == 0 else rows
        return remote(r_tx.at[c, way, s, pl.ds(0, n), :], r_rx.at[c, way, s, pl.ds(0, n), :],
                      r_send.at[c, way], r_recv.at[c, way, s], ahead[way])

    def q_copy(c, way, s):
        rs = res_rows(chip - sign[way] * s, core, way if s == hops - 1 else None)
        return remote(res.at[c, rs, :], res.at[c, rs, :], q_send.at[c, way], q_recv.at[c, way, s], ahead[way])

    def f_copy(c, rs):
        return remote(res.at[c, rs, :], res.at[c, rs, :], f_send.at[c], f_recv.at[c], partner)

    def stage_exchange(c):
        x_copy(c).wait_recv()
        own[c] = own[c] + x_rx[c].astype(F32)
        for way in range(2):
            r_tx[c, way, 0, pl.ds(0, h), :] = own[c, shard(chip + hops, way), :].astype(BF16)
            r_copy(c, way, 0).start()

    def stage_reduce(s):
        def run(c):
            for way in range(2):
                r_copy(c, way, s - 1).wait_recv()
                z = chip + sign[way] * (hops - s)
                if s == 1:
                    r_tx[c, way, s, pl.ds(way * h, h), :] = (
                        own[c, shard(z, way), :] + r_rx[c, way, 0, pl.ds(0, h), :].astype(F32)).astype(BF16)
                    r_tx[c, way, s, pl.ds((1 - way) * h, h), :] = own[c, shard(z, 1 - way), :].astype(BF16)
                else:
                    r_tx[c, way, s] = (own[c, shard(z), :] + r_rx[c, way, s - 1].astype(F32)).astype(BF16)
                r_copy(c, way, s).start()
        return run

    def stage_finish(c):
        for way in range(2):
            r_copy(c, way, hops - 1).wait_recv()
        total = own[c, shard(chip), :] + r_rx[c, 0, hops - 1].astype(F32) + r_rx[c, 1, hops - 1].astype(F32)
        res[c, res_rows(chip, core), :] = total.astype(BF16)
        for way in range(2):
            q_copy(c, way, 0).start()
        f_copy(c, res_rows(chip, core)).start()

    def stage_gather(s):
        def run(c):
            for way in range(2):
                rs = res_rows(chip - sign[way] * s, core, way if s == hops else None)
                remote(res.at[c, rs, :], res.at[c, rs, :], q_send.at[c, way], q_recv.at[c, way, s - 1],
                       ahead[way]).wait_recv()
                if s < hops:
                    q_copy(c, way, s).start()
                f_copy(c, rs).start()
        return run

    def stage_out(c):
        f_copy(c, half_rows(1 - core)).wait_recv()
        o_copy(c).start()

    stages = [stage_exchange, *[stage_reduce(s) for s in range(1, hops)], stage_finish,
              *[stage_gather(s) for s in range(1, hops + 1)], stage_out]

    def piece(c):
        n, j = c // per, lax.rem(c, per)
        s = lax.rem(c, DEPTH)

        @pl.when(c + DEPTH - 1 < pieces)
        def _():
            each(0, steps, lambda k: g_copy(c + DEPTH - 1, k).start())

        @pl.when(j == 0)
        def _():
            def step(k):
                a_copy(n, k).wait()
                g_copy(c, k).wait()
                ks = pl.ds(pl.multiple_of(k * TOKS, TOKS), TOKS)
                t = a_in[ks, :].T
                a_t[:, ks] = t
                part = jnp.dot(t, g_in[s, ks, :], preferred_element_type=F32)

                @pl.when(k == 0)
                def _():
                    acc[...] = part

                @pl.when(k > 0)
                def _():
                    acc[...] += part
            each(0, steps, step)

        @pl.when(j > 0)
        def _():
            each(0, steps, lambda k: g_copy(c, k).wait())

            @pl.when((j == 1) & (n + 1 < mats))
            def _():
                each(0, steps, lambda k: a_copy(n + 1, k).start())
            acc[...] = jnp.dot(a_t[...], g_in[s], preferred_element_type=F32)

        x_tx[c] = acc[half_rows(1 - core), :].astype(BF16)
        x_copy(c).start()
        own[c] = acc[half_rows(core), :]

    def first(k):
        a_copy(0, k).start()
        g_copy(0, k).start()
    each(0, steps, first)
    for c in range(1, DEPTH - 1):
        each(0, steps, lambda k: g_copy(c, k).start())

    def tick(t):
        @pl.when(t < pieces)
        def _():
            piece(t)
        for i, stage in enumerate(stages):
            c = t - 1 - LAG * i

            @pl.when((c >= 0) & (c < pieces))
            def _(stage=stage, c=c):
                stage(c)
    each(0, pieces + 1 + LAG * (len(stages) - 1), tick)

    sent = (2 * hops - 1) * h

    def drain(c):
        x_copy(c).wait_send()
        for way in range(2):
            part = x_tx.at[c, pl.ds(0, sent), :]
            remote(part, part, r_send.at[c, way], r_recv.at[c, way, 0], ahead[way]).wait_send()
            remote(part, part, q_send.at[c, way], q_recv.at[c, way, 0], ahead[way]).wait_send()
        f_copy(c, half_rows(core)).wait_send()
        o_copy(c).wait()
    each(0, pieces, drain)


def solution(mesh):
    chips = mesh.shape["dp"] // 2
    spec = jax.sharding.PartitionSpec

    def local(a, g):
        a, g = a[0], g[0]
        mats, toks, d = a.shape
        ff = g.shape[2]
        pieces, steps = mats * (ff // COLS), toks // TOKS
        half, rows, hops = d // 2, d // 2 // chips, chips // 2
        dma = pltpu.SemaphoreType.DMA
        return pl.pallas_call(
            functools.partial(sums_kernel, chips),
            out_shape=jax.ShapeDtypeStruct((mats, d, ff), BF16),
            in_specs=[pl.BlockSpec(memory_space=pl.ANY)] * 2,
            out_specs=pl.BlockSpec(memory_space=pl.ANY),
            scratch_shapes=[
                pltpu.VMEM((toks, d), BF16),
                pltpu.VMEM((d, toks), BF16),
                pltpu.VMEM((DEPTH, toks, COLS), BF16),
                pltpu.VMEM((d, COLS), F32),
                pltpu.VMEM((pieces, half, COLS), F32),
                pltpu.VMEM((pieces, half, COLS), BF16),
                pltpu.VMEM((pieces, half, COLS), BF16),
                pltpu.VMEM((pieces, 2, hops, rows, COLS), BF16),
                pltpu.VMEM((pieces, 2, hops, rows, COLS), BF16),
                pltpu.VMEM((pieces, d, COLS), BF16),
                dma((steps,)), dma((DEPTH, steps)), dma((pieces,)),
                dma((pieces,)), dma((pieces,)),
                dma((pieces, 2)), dma((pieces, 2, hops)),
                dma((pieces, 2)), dma((pieces, 2, hops)),
                dma((pieces,)), dma((pieces,)),
            ],
            compiler_params=pltpu.CompilerParams(
                collective_id=0, has_side_effects=True, vmem_limit_bytes=63 * 2**20),
            cost_estimate=pl.CostEstimate(
                flops=2 * mats * toks * d * ff, transcendentals=0,
                bytes_accessed=2 * mats * (toks * (d + ff) + d * ff)),
            name="sums",
        )(a, g)

    return jax.shard_map(local, mesh=mesh, in_specs=(spec(("rep", "dp")), spec(("rep", "dp"))),
                         out_specs=spec("rep"), check_vma=False)
```

```python
import functools

import jax
import jax.numpy as jnp
from jax import lax
from jax.experimental import pallas as pl
from jax.experimental.pallas import tpu as pltpu

BF16, F32 = jnp.bfloat16, jnp.float32
COLS = 256
TOKS = 2048
DEPTH = 3
SUM_LAG = 3
SHARE_LAG = 3


def sums_kernel(chips, a_ref, g_ref, res, a_in, a_t, g_in, acc, own, x_tx, x_rx, r_tx, r_rx,
                a_sem, g_sem, x_send, x_recv, r_send, r_recv, q_send, q_recv, f_send, f_recv):
    mats, toks, d = a_ref.shape
    per = g_ref.shape[2] // COLS
    steps = toks // TOKS
    pieces = mats * per
    half = d // 2
    rows = half // chips
    hops = chips // 2
    mid = hops // 2

    rep, me = lax.axis_index("rep"), lax.axis_index("dp")
    chip, core = me // 2, lax.rem(me, 2)

    def at(z, c):
        return (rep, lax.rem(z + chips, chips) * 2 + c)

    partner, up, down = at(chip, 1 - core), at(chip + 1, core), at(chip - 1, core)
    ahead = (up, down)
    sign = (1, -1)

    def remote(src, dst, ss, rs, dev):
        return pltpu.make_async_remote_copy(src_ref=src, dst_ref=dst, send_sem=ss, recv_sem=rs, device_id=dev,
                                            device_id_type=pl.DeviceIdType.MESH)

    def each(lo, hi, f):
        def body(i, carry):
            f(i)
            return carry
        lax.fori_loop(lo, hi, body, 0)

    def a_copy(n, k):
        ks = pl.ds(pl.multiple_of(k * TOKS, TOKS), TOKS)
        return pltpu.make_async_copy(a_ref.at[n, ks, :], a_in.at[ks, :], a_sem.at[k])

    def g_copy(c, k):
        ks = pl.ds(pl.multiple_of(k * TOKS, TOKS), TOKS)
        cs = pl.ds(pl.multiple_of((c % per) * COLS, COLS), COLS)
        s = lax.rem(c, DEPTH)
        return pltpu.make_async_copy(g_ref.at[c // per, ks, cs], g_in.at[s, ks, :], g_sem.at[s, k])

    def done(c, rs):
        cs = pl.ds(pl.multiple_of((c % per) * COLS, COLS), COLS)
        return res.at[c // per, rs, cs]

    def half_rows(which):
        return pl.ds(pl.multiple_of(which * half, half), half)

    def shard(z, part=None):
        z = lax.rem(z + chips, chips)
        n = rows if part is None else rows // 2
        return pl.ds(pl.multiple_of(z * rows + (0 if part is None else part * n), n), n)

    def res_rows(z, c, part=None):
        z = lax.rem(z + chips, chips)
        n = rows if part is None else rows // 2
        return pl.ds(pl.multiple_of(c * half + z * rows + (0 if part is None else part * n), n), n)

    h = rows // 2

    def landed(sem, n):
        part = x_rx.at[0, pl.ds(0, n), :]
        remote(part, part, x_send.at[0], sem, partner).wait_recv()

    def x_copy(c):
        return remote(x_tx.at[c], x_rx.at[c], x_send.at[c], x_recv.at[c], partner)

    def r_copy(c, way, s):
        n = h if s == 0 else rows
        return remote(r_tx.at[c, way, s, pl.ds(0, n), :], r_rx.at[c, way, s, pl.ds(0, n), :],
                      r_send.at[c], r_recv.at[c, s], ahead[way])

    def q_copy(c, way, gap, ahead_by):
        far = gap + ahead_by
        rs = res_rows(chip - sign[way] * gap, core, way if far == hops else None)
        return remote(done(c, rs), done(c, rs), q_send.at[c], q_recv.at[c, 1 if far == mid else 0],
                      at(chip + sign[way] * ahead_by, core))

    def f_copy(c, rs):
        return remote(done(c, rs), done(c, rs), f_send.at[c], f_recv.at[c], partner)

    def stage_exchange(c):
        x_copy(c).wait_recv()
        own[c] = own[c] + x_rx[c].astype(F32)
        for way in range(2):
            r_tx[c, way, 0, pl.ds(0, h), :] = own[c, shard(chip + hops, way), :].astype(BF16)
            r_copy(c, way, 0).start()

    def stage_reduce(s):
        def run(c):
            landed(r_recv.at[c, s - 1], 2 * (h if s == 1 else rows))
            for way in range(2):
                z = chip + sign[way] * (hops - s)
                if s == 1:
                    r_tx[c, way, s, pl.ds(way * h, h), :] = (
                        own[c, shard(z, way), :] + r_rx[c, way, 0, pl.ds(0, h), :].astype(F32)).astype(BF16)
                    r_tx[c, way, s, pl.ds((1 - way) * h, h), :] = own[c, shard(z, 1 - way), :].astype(BF16)
                else:
                    r_tx[c, way, s] = (own[c, shard(z), :] + r_rx[c, way, s - 1].astype(F32)).astype(BF16)
                r_copy(c, way, s).start()
        return run

    def stage_finish(c):
        landed(r_recv.at[c, hops - 1], 2 * rows)
        total = own[c, shard(chip), :] + r_rx[c, 0, hops - 1].astype(F32) + r_rx[c, 1, hops - 1].astype(F32)
        done(c, res_rows(chip, core))[...] = total.astype(BF16)
        for d in range(mid, 0, -1):
            for way in range(2):
                q_copy(c, way, 0, d).start()

    def stage_forward(c):
        landed(q_recv.at[c, 1], 2 * rows)
        for way in range(2):
            for d in range(hops - mid, 0, -1):
                q_copy(c, way, mid, d).start()

    def stage_settle(c):
        landed(q_recv.at[c, 0], half - 3 * rows)
        f_copy(c, half_rows(core)).start()

    def stage_out(c):
        f_copy(c, half_rows(1 - core)).wait_recv()

    stages = [(stage_exchange, 2)]
    for s in range(1, hops):
        stages.append((stage_reduce(s), stages[-1][1] + SUM_LAG))
    stages.append((stage_finish, stages[-1][1] + SUM_LAG))
    stages.append((stage_forward, stages[-1][1] + SHARE_LAG))
    stages.append((stage_settle, stages[-1][1] + SHARE_LAG))
    stages.append((stage_out, stages[-1][1] + 2))
    ticks = pieces + stages[-1][1] // 2

    def run(phase, t):
        for stage, place in stages[1:] + stages[:1]:
            if place % 2 != phase:
                continue
            c = t - place // 2

            @pl.when((c >= 0) & (c < pieces))
            def _(stage=stage, c=c):
                stage(c)

    def fetch(c):
        @pl.when(c + DEPTH - 1 < pieces)
        def _():
            each(0, steps, lambda k: g_copy(c + DEPTH - 1, k).start())

    def piece_first(c, lo, hi):
        n, s = c // per, lax.rem(c, DEPTH)

        def step(k):
            a_copy(n, k).wait()
            g_copy(c, k).wait()
            ks = pl.ds(pl.multiple_of(k * TOKS, TOKS), TOKS)
            t = a_in[ks, :].T
            a_t[:, ks] = t
            part = jnp.dot(t, g_in[s, ks, :], preferred_element_type=F32)

            @pl.when(k == 0)
            def _():
                acc[...] = part

            @pl.when(k > 0)
            def _():
                acc[...] += part
        each(lo, hi, step)

    def first_terms(c):
        x_tx[c] = acc[half_rows(1 - core), :].astype(BF16)
        x_copy(c).start()
        own[c] = acc[half_rows(core), :]

    def piece_other(c):
        n, j, s = c // per, lax.rem(c, per), lax.rem(c, DEPTH)
        each(0, steps, lambda k: g_copy(c, k).wait())

        @pl.when((j == 1) & (n + 1 < mats))
        def _():
            each(0, steps, lambda k: a_copy(n + 1, k).start())
        x_tx[c] = jnp.dot(a_t[half_rows(1 - core), :], g_in[s], preferred_element_type=F32).astype(BF16)
        x_copy(c).start()

    def piece_own(c):
        s = lax.rem(c, DEPTH)
        own[c] = jnp.dot(a_t[half_rows(core), :], g_in[s], preferred_element_type=F32)

    barrier = pltpu.get_barrier_semaphore()
    others = [partner, *[at(chip + w * k, core) for k in range(1, mid + 1) for w in sign]]
    for dev in others:
        pl.semaphore_signal(barrier, inc=1, device_id=dev, device_id_type=pl.DeviceIdType.MESH)

    def first(k):
        a_copy(0, k).start()
        g_copy(0, k).start()
    each(0, steps, first)
    piece_first(0, 0, steps // 2)
    for c in range(1, DEPTH - 1):
        each(0, steps, lambda k: g_copy(c, k).start())
    piece_first(0, steps // 2, steps)
    fetch(0)
    pl.semaphore_wait(barrier, len(others))
    first_terms(0)

    def tick(t):
        more = t < pieces
        later = more & (lax.rem(t, per) > 0)
        newer = more & (lax.rem(t, per) == 0)

        @pl.when(more)
        def _():
            fetch(t)

        @pl.when(newer)
        def _():
            piece_first(t, 0, steps // 2)

        @pl.when(later)
        def _():
            piece_other(t)
        run(0, t)

        @pl.when(newer)
        def _():
            piece_first(t, steps // 2, steps)
            first_terms(t)

        @pl.when(later)
        def _():
            piece_own(t)
        run(1, t)
    each(1, ticks, tick)

    def drain(c):
        x_copy(c).wait_send()
        part = x_tx.at[c, pl.ds(0, half - rows), :]
        remote(part, part, r_send.at[c], r_recv.at[c, 0], partner).wait_send()
        remote(part, part, q_send.at[c], q_recv.at[c, 0], partner).wait_send()
        f_copy(c, half_rows(core)).wait_send()
    each(0, pieces, drain)


def solution(mesh):
    chips = mesh.shape["dp"] // 2
    spec = jax.sharding.PartitionSpec

    def local(a, g):
        a, g = a[0], g[0]
        mats, toks, d = a.shape
        ff = g.shape[2]
        pieces, steps = mats * (ff // COLS), toks // TOKS
        half, rows, hops = d // 2, d // 2 // chips, chips // 2
        dma = pltpu.SemaphoreType.DMA
        return pl.pallas_call(
            functools.partial(sums_kernel, chips),
            out_shape=pltpu.VMEM((mats, d, ff), BF16),
            in_specs=[pl.BlockSpec(memory_space=pl.ANY)] * 2,
            out_specs=pl.BlockSpec(memory_space=pltpu.VMEM),
            scratch_shapes=[
                pltpu.VMEM((toks, d), BF16),
                pltpu.VMEM((d, toks), BF16),
                pltpu.VMEM((DEPTH, toks, COLS), BF16),
                pltpu.VMEM((d, COLS), F32),
                pltpu.VMEM((pieces, half, COLS), F32),
                pltpu.VMEM((pieces, half, COLS), BF16),
                pltpu.VMEM((pieces, half, COLS), BF16),
                pltpu.VMEM((pieces, 2, hops, rows, COLS), BF16),
                pltpu.VMEM((pieces, 2, hops, rows, COLS), BF16),
                dma((steps,)), dma((DEPTH, steps)),
                dma((pieces,)), dma((pieces,)),
                dma((pieces,)), dma((pieces, hops)),
                dma((pieces,)), dma((pieces, 2)),
                dma((pieces,)), dma((pieces,)),
            ],
            compiler_params=pltpu.CompilerParams(
                collective_id=0, has_side_effects=True, vmem_limit_bytes=52 * 2**20),
            cost_estimate=pl.CostEstimate(
                flops=2 * mats * toks * d * ff, transcendentals=0,
                bytes_accessed=2 * mats * (toks * (d + ff) + d * ff)),
            name="sums",
        )(a, g)

    return jax.shard_map(local, mesh=mesh, in_specs=(spec(("rep", "dp")), spec(("rep", "dp"))),
                         out_specs=spec("rep"), check_vma=False)
```

```python
import functools

import jax
import jax.numpy as jnp
from jax import lax
from jax.experimental import pallas as pl
from jax.experimental.pallas import tpu as pltpu

BF16, F32 = jnp.bfloat16, jnp.float32
COLS = 256
TOKS = 4096
DEPTH = 3
SUM_LAG = 3
SHARE_LAG = 3


def sums_kernel(chips, a_ref, g_ref, res, a_in, a_t, g_in, acc, own, x_tx, x_rx, r_tx, r_rx,
                a_sem, g_sem, x_send, x_recv, r_send, r_recv, q_send, q_recv, f_send, f_recv):
    mats, toks, d = a_ref.shape
    per = g_ref.shape[2] // COLS
    steps = toks // TOKS
    pieces = mats * per
    half = d // 2
    rows = half // chips
    hops = chips // 2
    mid = hops // 2

    rep, me = lax.axis_index("rep"), lax.axis_index("dp")
    chip, core = me // 2, lax.rem(me, 2)

    def at(z, c):
        return (rep, lax.rem(z + chips, chips) * 2 + c)

    partner, up, down = at(chip, 1 - core), at(chip + 1, core), at(chip - 1, core)
    ahead = (up, down)
    sign = (1, -1)

    def remote(src, dst, ss, rs, dev):
        return pltpu.make_async_remote_copy(src_ref=src, dst_ref=dst, send_sem=ss, recv_sem=rs, device_id=dev,
                                            device_id_type=pl.DeviceIdType.MESH)

    def each(lo, hi, f):
        def body(i, carry):
            f(i)
            return carry
        lax.fori_loop(lo, hi, body, 0)

    def a_copy(n, k):
        ks = pl.ds(pl.multiple_of(k * TOKS, TOKS), TOKS)
        return pltpu.make_async_copy(a_ref.at[n, ks, :], a_in.at[ks, :], a_sem.at[k])

    def g_copy(c, k):
        ks = pl.ds(pl.multiple_of(k * TOKS, TOKS), TOKS)
        cs = pl.ds(pl.multiple_of((c % per) * COLS, COLS), COLS)
        s = lax.rem(c, DEPTH)
        return pltpu.make_async_copy(g_ref.at[c // per, ks, cs], g_in.at[s, ks, :], g_sem.at[s, k])

    def done(c, rs):
        cs = pl.ds(pl.multiple_of((c % per) * COLS, COLS), COLS)
        return res.at[c // per, rs, cs]

    def half_rows(which):
        return pl.ds(pl.multiple_of(which * half, half), half)

    def shard(z, part=None):
        z = lax.rem(z + chips, chips)
        n = rows if part is None else rows // 2
        return pl.ds(pl.multiple_of(z * rows + (0 if part is None else part * n), n), n)

    def res_rows(z, c, part=None):
        z = lax.rem(z + chips, chips)
        n = rows if part is None else rows // 2
        return pl.ds(pl.multiple_of(c * half + z * rows + (0 if part is None else part * n), n), n)

    h = rows // 2

    def landed(sem, n):
        part = x_rx.at[0, pl.ds(0, n), :]
        remote(part, part, x_send.at[0], sem, partner).wait_recv()

    def x_copy(c):
        return remote(x_tx.at[c], x_rx.at[c], x_send.at[c], x_recv.at[c], partner)

    def r_copy(c, way, s):
        n = h if s == 0 else rows
        return remote(r_tx.at[c, way, s, pl.ds(0, n), :], r_rx.at[c, way, s, pl.ds(0, n), :],
                      r_send.at[c], r_recv.at[c, s], ahead[way])

    def q_copy(c, way, gap, ahead_by):
        far = gap + ahead_by
        rs = res_rows(chip - sign[way] * gap, core, way if far == hops else None)
        return remote(done(c, rs), done(c, rs), q_send.at[c], q_recv.at[c, 1 if far == mid else 0],
                      at(chip + sign[way] * ahead_by, core))

    def f_copy(c, rs):
        return remote(done(c, rs), done(c, rs), f_send.at[c], f_recv.at[c], partner)

    def stage_exchange(c):
        x_copy(c).wait_recv()
        own[c] = own[c] + x_rx[c].astype(F32)
        for way in range(2):
            r_tx[c, way, 0, pl.ds(0, h), :] = own[c, shard(chip + hops, way), :].astype(BF16)
            r_copy(c, way, 0).start()

    def stage_reduce(s):
        def run(c):
            landed(r_recv.at[c, s - 1], 2 * (h if s == 1 else rows))
            for way in range(2):
                z = chip + sign[way] * (hops - s)
                if s == 1:
                    r_tx[c, way, s, pl.ds(way * h, h), :] = (
                        own[c, shard(z, way), :] + r_rx[c, way, 0, pl.ds(0, h), :].astype(F32)).astype(BF16)
                    r_tx[c, way, s, pl.ds((1 - way) * h, h), :] = own[c, shard(z, 1 - way), :].astype(BF16)
                else:
                    r_tx[c, way, s] = (own[c, shard(z), :] + r_rx[c, way, s - 1].astype(F32)).astype(BF16)
                r_copy(c, way, s).start()
        return run

    def stage_finish(c):
        landed(r_recv.at[c, hops - 1], 2 * rows)
        total = own[c, shard(chip), :] + r_rx[c, 0, hops - 1].astype(F32) + r_rx[c, 1, hops - 1].astype(F32)
        done(c, res_rows(chip, core))[...] = total.astype(BF16)
        for d in range(mid, 0, -1):
            for way in range(2):
                q_copy(c, way, 0, d).start()

    def stage_forward(c):
        landed(q_recv.at[c, 1], 2 * rows)
        for way in range(2):
            for d in range(hops - mid, 0, -1):
                q_copy(c, way, mid, d).start()

    def stage_settle(c):
        landed(q_recv.at[c, 0], half - 3 * rows)
        f_copy(c, half_rows(core)).start()

    def stage_out(c):
        f_copy(c, half_rows(1 - core)).wait_recv()

    stages = [(stage_exchange, 2)]
    for s in range(1, hops):
        stages.append((stage_reduce(s), stages[-1][1] + SUM_LAG))
    stages.append((stage_finish, stages[-1][1] + SUM_LAG))
    stages.append((stage_forward, stages[-1][1] + SHARE_LAG))
    stages.append((stage_settle, stages[-1][1] + SHARE_LAG))
    stages.append((stage_out, stages[-1][1] + 2))
    ticks = pieces + stages[-1][1] // 2

    def run(phase, t):
        for stage, place in stages[1:] + stages[:1]:
            if place % 2 != phase:
                continue
            c = t - place // 2

            @pl.when((c >= 0) & (c < pieces))
            def _(stage=stage, c=c):
                stage(c)

    def fetch(c):
        @pl.when(c + DEPTH - 1 < pieces)
        def _():
            each(0, steps, lambda k: g_copy(c + DEPTH - 1, k).start())

    def piece_first(c, lo, hi):
        n, s = c // per, lax.rem(c, DEPTH)

        def step(k):
            a_copy(n, k).wait()
            g_copy(c, k).wait()
            ks = pl.ds(pl.multiple_of(k * TOKS, TOKS), TOKS)
            t = a_in[ks, :].T
            a_t[:, ks] = t
            part = jnp.dot(t, g_in[s, ks, :], preferred_element_type=F32)

            @pl.when(k == 0)
            def _():
                acc[...] = part

            @pl.when(k > 0)
            def _():
                acc[...] += part
        each(lo, hi, step)

    def first_terms(c):
        x_tx[c] = acc[half_rows(1 - core), :].astype(BF16)
        x_copy(c).start()
        own[c] = acc[half_rows(core), :]

    def piece_other(c):
        n, j, s = c // per, lax.rem(c, per), lax.rem(c, DEPTH)
        each(0, steps, lambda k: g_copy(c, k).wait())

        @pl.when((j == 1) & (n + 1 < mats))
        def _():
            each(0, steps, lambda k: a_copy(n + 1, k).start())
        x_tx[c] = jnp.dot(a_t[half_rows(1 - core), :], g_in[s], preferred_element_type=F32).astype(BF16)
        x_copy(c).start()

    def piece_own(c):
        s = lax.rem(c, DEPTH)
        own[c] = jnp.dot(a_t[half_rows(core), :], g_in[s], preferred_element_type=F32)

    barrier = pltpu.get_barrier_semaphore()
    others = [partner, *[at(chip + w * k, core) for k in range(1, mid + 1) for w in sign]]
    for dev in others:
        pl.semaphore_signal(barrier, inc=1, device_id=dev, device_id_type=pl.DeviceIdType.MESH)

    def first(k):
        a_copy(0, k).start()
        g_copy(0, k).start()
    each(0, steps, first)
    piece_first(0, 0, steps // 2)
    for c in range(1, DEPTH - 1):
        each(0, steps, lambda k: g_copy(c, k).start())
    piece_first(0, steps // 2, steps)
    fetch(0)
    pl.semaphore_wait(barrier, len(others))
    first_terms(0)

    def tick(t):
        more = t < pieces
        later = more & (lax.rem(t, per) > 0)
        newer = more & (lax.rem(t, per) == 0)

        @pl.when(more)
        def _():
            fetch(t)

        @pl.when(newer)
        def _():
            piece_first(t, 0, steps // 2)

        @pl.when(later)
        def _():
            piece_other(t)
        run(0, t)

        @pl.when(newer)
        def _():
            piece_first(t, steps // 2, steps)
            first_terms(t)

        @pl.when(later)
        def _():
            piece_own(t)
        run(1, t)
    each(1, ticks, tick)

    def drain(c):
        x_copy(c).wait_send()
        part = x_tx.at[c, pl.ds(0, half - rows), :]
        remote(part, part, r_send.at[c], r_recv.at[c, 0], partner).wait_send()
        remote(part, part, q_send.at[c], q_recv.at[c, 0], partner).wait_send()
        f_copy(c, half_rows(core)).wait_send()
    each(0, pieces, drain)


def solution(mesh):
    chips = mesh.shape["dp"] // 2
    spec = jax.sharding.PartitionSpec

    def local(a, g):
        a, g = a[0], g[0]
        mats, toks, d = a.shape
        ff = g.shape[2]
        pieces, steps = mats * (ff // COLS), toks // TOKS
        half, rows, hops = d // 2, d // 2 // chips, chips // 2
        dma = pltpu.SemaphoreType.DMA
        return pl.pallas_call(
            functools.partial(sums_kernel, chips),
            out_shape=pltpu.VMEM((mats, d, ff), BF16),
            in_specs=[pl.BlockSpec(memory_space=pl.ANY)] * 2,
            out_specs=pl.BlockSpec(memory_space=pltpu.VMEM),
            scratch_shapes=[
                pltpu.VMEM((toks, d), BF16),
                pltpu.VMEM((d, toks), BF16),
                pltpu.VMEM((DEPTH, toks, COLS), BF16),
                pltpu.VMEM((d, COLS), F32),
                pltpu.VMEM((pieces, half, COLS), F32),
                pltpu.VMEM((pieces, half, COLS), BF16),
                pltpu.VMEM((pieces, half, COLS), BF16),
                pltpu.VMEM((pieces, 2, hops, rows, COLS), BF16),
                pltpu.VMEM((pieces, 2, hops, rows, COLS), BF16),
                dma((steps,)), dma((DEPTH, steps)),
                dma((pieces,)), dma((pieces,)),
                dma((pieces,)), dma((pieces, hops)),
                dma((pieces,)), dma((pieces, 2)),
                dma((pieces,)), dma((pieces,)),
            ],
            compiler_params=pltpu.CompilerParams(
                collective_id=0, has_side_effects=True, vmem_limit_bytes=52 * 2**20),
            cost_estimate=pl.CostEstimate(
                flops=2 * mats * toks * d * ff, transcendentals=0,
                bytes_accessed=2 * mats * (toks * (d + ff) + d * ff)),
            name="sums",
        )(a, g)

    return jax.shard_map(local, mesh=mesh, in_specs=(spec(("rep", "dp")), spec(("rep", "dp"))),
                         out_specs=spec("rep"), check_vma=False)
```
